32 devices in a mesh: section: 2 (over x), expert: 16 (over z, y, core).
Axes of the slice: x: 2, y: 2, z: 4, core: 2. Of those that a mesh axis runs over, the one named last changes fastest.
Arguments:
- hidden_in: bfloat16 [2, 128, 3584], P(None, 'expert'), may hold values from -6 to 6
- layer_gain: float32 [2, 3584], P('section'), may hold values from 0.25 to 1.75
- router: bfloat16 [2, 3584, 4], P('section'), may hold values from -0.09375 to 0.09375
- w_gate: bfloat16 [2, 3584, 8192], P('section', None, 'expert'), may hold values from -0.09375 to 0.09375
- w_up: bfloat16 [2, 3584, 8192], P('section', None, 'expert'), may hold values from -0.09375 to 0.09375
- w_down: bfloat16 [2, 8192, 3584], P('section', 'expert'), may hold values from -0.125 to 0.125
- final_gain: float32 [3584], replicated, may hold values from 0.25 to 1.75
- head: bfloat16 [8192, 3584], P(('section', 'expert')), may hold values from -18.775102 to 18.775102
- routing: int32 [2, 2, 128, 2], P('section', None, 'expert'), may hold values from 0 to 3, all different within a row; in each aligned block of 8 rows (0 to 7, 8 to 15, ..., all dimensions but the last counted through in order) at most 4 rows name the same one
- targets: int32 [2, 128], replicated, may hold values from 0 to 8191
- seq_ids: int32 [2, 128], replicated, may hold values from 0 to 3, never falling along the last dimension, each value on 1 to 64 neighbouring positions
Outputs:
- token_logprob: float32 [2, 128], P(None, 'expert')
- seq_mean: float32 [2, 4], replicated
The draws below stay inside these ranges and needn't reach their ends.
Inputs may be any that keep to these rules, and one draw needn't show every extreme that they name: `routing`: in each aligned block of 8 tokens (the tokens of one device) a token's 2 experts differ and no expert is named by more than 4 tokens; some expert is named by exactly 4. `seq_ids`: ids never fall along a micro-batch's tokens; each of the 4 ids occurs on 1 to 64 tokens, one on exactly 64.
All inputs are finite; a program needn't handle non-finite values.
Results may differ from the reference program's by a relative error of at most 0.014.
Values may be sent and summed in bfloat16 or wider, within the bound.
A program may use at most 64 MiB of HBM per device.

```python
import math
import jax
import jax.numpy as jnp
import numpy as np
from jax import lax

D = 3584
FF = 2048
FF_SPLIT = 4
TOP = 2
TOK_DEV = 8
MICRO = 2
SEQS = 4
LAYERS = 2
EXPERTS = 4
FF_DEV = 512
TOKENS = 128
VOCAB = 8192
CAP = 4
SEQ_MOST = 64
N_EXPERT = 16


def draw_head(key, part):
    keys = jax.random.split(jax.random.fold_in(key, 17), 2)
    base = jnp.clip(jax.random.normal(keys[0], (VOCAB, D), jnp.float32), -4.0, 4.0)
    position = jnp.arange(VOCAB, dtype=jnp.float32)[:, None] / VOCAB
    rising = 0.6 + 1.2 * position
    jitter = jax.random.uniform(keys[1], (VOCAB, 1), jnp.float32, 0.7, 1.3)
    values = base * (3.0 / math.sqrt(D)) * rising * jitter
    return values.astype(jnp.bfloat16)


def plant(array, rng, low, top_value):
    longest = array.shape.index(max(array.shape))
    spots = []
    for shift in (0, 1):
        where = [jax.random.randint(jax.random.fold_in(rng, axis), (), 0, length) for axis, length in enumerate(array.shape)]
        where[longest] = (where[longest] + shift) % array.shape[longest]
        spots.append(tuple(where))
    return array.at[spots[0]].set(low).at[spots[1]].set(top_value)


def block_scale(own_key, dims, cuts, low, high):
    level = 1.0
    for dim, blocks in cuts:
        steps = jax.random.uniform(jax.random.fold_in(jax.random.fold_in(own_key, 6), dim), (blocks,), jnp.float32, low / len(cuts), high / len(cuts))
        level = level * jnp.repeat(jnp.exp(steps), dims[dim] // blocks).reshape((-1,) + (1,) * (len(dims) - 1 - dim))
    return level


def cumulative_ranks(number_of, lean):
    loads = [(1 << 20) // math.isqrt(rank ** lean) + 1 for rank in range(1, number_of + 1)]
    deviation = 1 + sum(loads) // (1 << 30)
    return np.cumsum(np.array([max(1, weight // deviation) for weight in loads]))


def ranked(own_key, shape, number_of, slope):
    grid = cumulative_ranks(number_of, slope)
    pick = jax.random.randint(jax.random.fold_in(own_key, 1), shape, 0, int(grid[number_of - 1]))
    grade = jnp.searchsorted(jnp.asarray(grid, jnp.int32), pick, side="right")
    return jax.random.permutation(jax.random.fold_in(own_key, 2), number_of)[grade].astype(jnp.int32)


def split_up(amount, total, most, lean):
    loads = [(1 << 20) // math.isqrt(grade ** lean) + 1 for grade in range(2, amount + 1)]
    surplus, holding = total - most - (amount - 1), [1] * (amount - 1)
    while surplus > 0:
        movable = [i for i in range(amount - 1) if holding[i] < most]
        whole, left = sum([loads[i] for i in movable]), surplus
        for i in movable:
            extra = min(most - holding[i], max(1, left * loads[i] // whole), surplus)
            holding[i] = holding[i] + extra
            surplus = surplus - extra
    return np.array([most] + holding)


def ragged(rng, number_of, total, reach, skew):
    if number_of == 2:
        one = jax.random.randint(rng, (), max(1, total - reach), min(reach, total - 1) + 1)
        return jnp.stack([one, total - one])
    lengths = jnp.asarray(split_up(number_of, total, reach, skew), jnp.int32)
    twos = (number_of - 1) // 2
    giver, taker = lengths[1:1 + 2 * twos:2], lengths[2:2 + 2 * twos:2]
    slack = jnp.minimum(giver - 1, reach - taker)
    shifted = jax.random.randint(jax.random.fold_in(rng, 1), (twos,), 0, 1 << 20) % (slack + 1)
    lengths = lengths.at[1:1 + 2 * twos:2].set(giver - shifted).at[2:2 + 2 * twos:2].set(taker + shifted)
    return lengths[jax.random.permutation(jax.random.fold_in(rng, 2), number_of)]


def routed_block(key, own, number, rows, number_of, top, most, slope):
    order = jax.random.permutation(key, number_of)
    heavy_load, common = portions_of(number_of, rows * top, most, slope, True), portions_of(number_of, rows * top, most, slope, False)
    places = jnp.arange(number_of)

    def named(lengths, rotation):
        used = int((lengths > 0).sum())
        fixed = max(1, used // 4)
        shifted = fixed + (places - fixed + rotation * (used - fixed)) % max(1, number_of - fixed)
        return jnp.zeros((number_of,), jnp.int32).at[order[jnp.where(places < fixed, places, shifted)]].set(jnp.asarray(lengths, jnp.int32))

    lengths = jnp.where(number % 4 == 0, named(heavy_load, number // 4), named(common, number - number // 4 - 1))
    mixed = jax.random.permutation(jax.random.fold_in(own, 3), number_of)
    source_of, receiver = mixed[0:number_of // 2 * 2:2], mixed[1:number_of // 2 * 2:2]
    slack = jnp.minimum(lengths[source_of] - 1, most - lengths[receiver]) // 2
    slack = jnp.where((source_of == order[0]) | (receiver == order[0]) | (lengths[receiver] == 0), 0, jnp.maximum(slack, 0))
    shifted = jax.random.randint(jax.random.fold_in(own, 4), (number_of // 2,), 0, 1 << 20) % (slack + 1)
    lengths = lengths.at[source_of].add(-shifted).at[receiver].add(shifted)
    labels = jnp.searchsorted(jnp.cumsum(lengths), jnp.arange(rows * top), side="right").astype(jnp.int32)
    grid = labels.reshape(top, rows).T
    grid = grid[jax.random.permutation(jax.random.fold_in(own, 1), rows)]
    rotation = jax.random.randint(jax.random.fold_in(own, 2), (rows, 1), 0, top)
    return jnp.take_along_axis(grid, (jnp.arange(top)[None, :] + rotation) % top, axis=1)


def portions_of(count, total, most, slope, full):
    loads = [(1 << 20) // math.isqrt(standing ** slope) + 1 for standing in range(1, count + 1)]
    largest = most if full else min(most, max(-(-total // count), total * loads[0] // sum(loads)))
    least = 1 if total - largest >= count - 1 else 0
    given, rest = [largest] + [least] * (count - 1), total - largest - least * (count - 1)
    while rest > 0:
        candidates = [i for i in range(1, count) if given[i] < largest] or [i for i in range(1, count) if given[i] < most]
        mass, left = sum([loads[i] for i in candidates]), rest
        for i in candidates:
            extra = min(most - given[i], max(1, left * loads[i] // mass), rest)
            given[i] = given[i] + extra
            rest = rest - extra
    return np.array(given)


def noise(key, extent, width, bound, cuts=(), held_as=jnp.bfloat16):
    level = block_scale(key, extent, cuts, -0.22, 0.18) if cuts else 1.0
    result = jax.random.normal(key, extent, jnp.float32) * width * level
    return jnp.minimum(jnp.maximum(result, -bound), bound).astype(held_as)


def setup_inputs(seed: int = 0) -> dict:
    streams_of = jax.random.split(jax.random.key(seed), 12)
    hidden_in = noise(streams_of[0], (MICRO, TOKENS, D), 1.0, 6.0, ((1, 16),))
    layer_gain = jnp.clip(1.0 + 0.15 * jax.random.normal(streams_of[1], (LAYERS, D), jnp.float32), 0.25, 1.75)
    router = noise(streams_of[2], (LAYERS, D, EXPERTS), D ** -0.5, 0.09375, ((0, 2),))
    w_gate = noise(streams_of[3], (LAYERS, D, EXPERTS * FF), D ** -0.5, 0.09375, ((0, 2), (2, 16)))
    w_up = noise(streams_of[4], (LAYERS, D, EXPERTS * FF), D ** -0.5, 0.09375, ((0, 2), (2, 16)))
    w_down = noise(streams_of[5], (LAYERS, EXPERTS * FF, D), FF ** -0.5, 0.125, ((0, 2), (1, 16)))
    final_gain = jnp.clip(1.0 + 0.15 * jax.random.normal(streams_of[6], (D,), jnp.float32), 0.25, 1.75)
    head = draw_head(jax.random.fold_in(streams_of[11], 71), 0)
    routing_keys = jax.random.split(jax.random.fold_in(streams_of[8], 1), LAYERS * MICRO * TOKENS // TOK_DEV)
    routing_turns = jax.random.permutation(jax.random.fold_in(streams_of[8], 3), LAYERS * MICRO * TOKENS // TOK_DEV)
    routing = jax.vmap(lambda own, number: routed_block(jax.random.fold_in(streams_of[8], 2), own, number, TOK_DEV, EXPERTS, TOP, CAP, 2))(routing_keys, routing_turns).reshape((LAYERS, MICRO, TOKENS, TOP))
    targets = plant(ranked(streams_of[9], (MICRO, TOKENS), VOCAB, 2), jax.random.fold_in(streams_of[9], 3), 0, VOCAB - 1).astype(jnp.int32)
    seq_ids = jax.vmap(lambda own: jnp.searchsorted(jnp.cumsum(ragged(own, SEQS, TOKENS, SEQ_MOST, 1)), jnp.arange(TOKENS), side="right"))(jax.random.split(streams_of[10], MICRO)).reshape((MICRO, TOKENS)).astype(jnp.int32)
    return dict(hidden_in=hidden_in, layer_gain=layer_gain, router=router, w_gate=w_gate, w_up=w_up, w_down=w_down, final_gain=final_gain, head=head, routing=routing, targets=targets, seq_ids=seq_ids)


def rms_scale(states, gain):
    values = states.astype(jnp.float32)
    factor = lax.rsqrt(lax.optimization_barrier(jnp.mean(values * values, -1, keepdims=True)) + 1e-06)
    return values * factor * gain.astype(jnp.float32)

def run_expert(operands):
    packed_rows, gate_cols, up_cols, down_rows = operands
    gate_val = jnp.dot(packed_rows, gate_cols, preferred_element_type=jnp.float32)
    up_val = jnp.dot(packed_rows, up_cols, preferred_element_type=jnp.float32)
    inner = (jax.nn.silu(gate_val) * up_val).astype(jnp.bfloat16)
    count = inner.shape[0]
    pieces = jnp.einsum('rfk,fkd->rfd', inner.reshape(count, FF_SPLIT, FF_DEV).astype(jnp.float32), down_rows.reshape(FF_SPLIT, FF_DEV, D).astype(jnp.float32), precision=lax.Precision.HIGHEST)
    rounded = lax.optimization_barrier(pieces.astype(jnp.bfloat16))
    return lax.optimization_barrier(jnp.sum(rounded.astype(jnp.float32), 1))

def pick_rows(block_out, slot_index):
    return block_out[slot_index]

def expert_layer(states, gain, router, gate_w, up_w, down_w, route_ids):
    blocks = N_EXPERT
    normed = rms_scale(states, gain).astype(jnp.bfloat16)
    logits = jnp.dot(normed, router, preferred_element_type=jnp.float32)
    chosen = route_ids[:, :, None] == jnp.arange(EXPERTS, dtype=jnp.int32)[None, None, :]
    affinity = jax.nn.sigmoid(lax.optimization_barrier(jnp.sum(jnp.where(chosen, logits[:, None, :], 0.0), -1)))
    weight = affinity / lax.optimization_barrier(jnp.sum(affinity, -1, keepdims=True))
    flags = chosen.reshape(blocks, TOK_DEV * TOP, EXPERTS).astype(jnp.int32)
    ranks = jnp.cumsum(flags, 1) - flags
    slot_ids = lax.optimization_barrier(jnp.sum(ranks * flags, -1)).reshape(blocks, TOK_DEV, TOP)
    target_slot = (route_ids.reshape(blocks, TOK_DEV, TOP) * CAP + slot_ids).astype(jnp.int32)
    places = jnp.arange(EXPERTS * CAP, dtype=jnp.int32)
    table = jnp.any(places[None, :, None, None] == target_slot[:, None], -1).astype(jnp.float32)
    packed = jnp.einsum('bst,btd->bsd', table, normed.reshape(blocks, TOK_DEV, D).astype(jnp.float32), precision=lax.Precision.HIGHEST).astype(jnp.bfloat16)
    per_expert = packed.reshape(blocks, EXPERTS, CAP, D).transpose(1, 0, 2, 3).reshape(EXPERTS, blocks * CAP, D)
    gate_e = gate_w.reshape(D, EXPERTS, FF).transpose(1, 0, 2)
    up_e = up_w.reshape(D, EXPERTS, FF).transpose(1, 0, 2)
    down_e = down_w.reshape(EXPERTS, FF, D)
    outputs = lax.map(run_expert, (per_expert, gate_e, up_e, down_e))
    by_block = outputs.reshape(EXPERTS, blocks, CAP, D).transpose(1, 0, 2, 3).reshape(blocks, EXPERTS * CAP, D)
    picked = jax.vmap(pick_rows)(by_block, target_slot)
    mixed = lax.optimization_barrier(jnp.sum(weight.reshape(blocks, TOK_DEV, TOP)[..., None] * picked, 2)).reshape(TOKENS, D)
    return (states.astype(jnp.float32) + 2.5 * mixed).astype(jnp.bfloat16)

def reference(hidden_in, layer_gain, router, w_gate, w_up, w_down, final_gain, head, routing, targets, seq_ids):
    states = [hidden_in[micro_id] for micro_id in range(MICRO)]
    for level in range(LAYERS):
        states = [expert_layer(states[micro_id], layer_gain[level], router[level], w_gate[level], w_up[level], w_down[level], routing[level, micro_id]) for micro_id in range(MICRO)]
    stacked = jnp.stack(states)
    normed = rms_scale(stacked, final_gain).astype(jnp.bfloat16).reshape(MICRO * TOKENS, D)
    logits = jnp.dot(normed, head.T, preferred_element_type=jnp.float32).reshape(MICRO, TOKENS, VOCAB)
    peak = lax.optimization_barrier(jnp.max(logits, -1))
    total = lax.optimization_barrier(jnp.sum(jnp.exp(logits - peak[..., None]), -1))
    target_logit = jnp.take_along_axis(logits, targets[..., None].astype(jnp.int32), -1)[..., 0]
    logprob = target_logit - (peak + jnp.log(total))
    member = seq_ids[:, :, None] == jnp.arange(SEQS, dtype=jnp.int32)[None, None, :]
    sums = lax.optimization_barrier(jnp.sum(jnp.where(member, logprob[..., None], 0.0), 1))
    counts = lax.optimization_barrier(jnp.sum(member.astype(jnp.float32), 1))
    return (logprob, sums / counts)
```

```python
import functools

import jax
import jax.numpy as jnp
from jax import lax
from jax.experimental import pallas as pl
from jax.experimental.pallas import tpu as pltpu
from jax.sharding import PartitionSpec as P

SEQS = 4
CHUNKS = 2
F32 = jnp.float32
BF16 = jnp.bfloat16


def rms_scale(states, gain):
    values = states.astype(F32)
    factor = lax.rsqrt(jnp.mean(values * values, -1, keepdims=True) + 1e-06)
    return values * factor * gain


def kernel(
    dims,
    hid, gain, router, wg_hbm, wu_hbm, wd_hbm, fgain, head_hbm, route, tgt, seq,
    tok_out, seq_out,
    wg, wu, wd, head, stin, stout, pack, xbuf, pf, pb, cr, qf, qb, yr, sb, ret, fin, nb, stats,
    loc, dz, dy, dc, rc, ry, rz, xs, xr, fs, fr, az, ay, ac, ss, sr,
):
    S, E, J, C, R, M, T, cap, K = dims
    F = J * C
    members = E * F
    N = S * members
    MT = M * T
    D = stin.shape[1]
    Dc = D // K
    NT = members * MT
    sec = lax.axis_index("section")
    mem = lax.axis_index("expert")
    e = mem // F
    j = (mem % F) // C
    c = mem % C
    me = sec * members + mem
    voc = head.shape[0]
    cols = [pl.ds(k * Dc, Dc) for k in range(K)]

    def member(pe, pj, pc):
        return pe * F + pj * C + pc

    def remote(src, dst, send, recv, section, target):
        return pltpu.make_async_remote_copy(
            src_ref=src, dst_ref=dst, send_sem=send, recv_sem=recv,
            device_id=(section, target), device_id_type=pl.DeviceIdType.MESH,
        )

    locals_ = [
        pltpu.make_async_copy(wg_hbm, wg, loc.at[0]),
        pltpu.make_async_copy(wu_hbm, wu, loc.at[1]),
        pltpu.make_async_copy(wd_hbm, wd, loc.at[2]),
        pltpu.make_async_copy(head_hbm, head, loc.at[3]),
    ]
    load_hid = pltpu.make_async_copy(hid, stin, loc.at[4])

    @pl.when(sec == 0)
    def _():
        load_hid.start()

    for copy in locals_:
        copy.start()

    barrier = pltpu.get_barrier_semaphore()

    def greet(d, carry):
        peer = (me + d) % N
        pl.semaphore_signal(
            barrier, inc=1, device_id=(peer // members, peer % members),
            device_id_type=pl.DeviceIdType.MESH,
        )
        return carry

    lax.fori_loop(1, N, greet, 0)

    lanes = lax.broadcasted_iota(jnp.int32, (MT, E * R), 1)
    rows = lax.broadcasted_iota(jnp.int32, (MT, E * R), 0)
    hit = route[:, 0:1] == lanes // R
    for k in range(1, route.shape[1]):
        hit = hit | (route[:, k : k + 1] == lanes // R)
    hit_f = hit.astype(F32)
    row_a = lax.broadcasted_iota(jnp.int32, (MT, MT), 0)
    row_b = lax.broadcasted_iota(jnp.int32, (MT, MT), 1)
    earlier = ((row_b < row_a) & (row_a // T == row_b // T)).astype(BF16)
    rank = jnp.dot(earlier, hit_f.astype(BF16), preferred_element_type=F32)
    place = rank + ((rows // T) * cap).astype(F32)
    table = jnp.where(hit & (place == (lanes % R).astype(F32)), 1.0, 0.0).astype(F32)

    pl.semaphore_wait(barrier, N - 1)

    sends = []

    @pl.when(sec == 0)
    def _():
        load_hid.wait()

    @pl.when(sec > 0)
    def _():
        for k in range(K):
            remote(stout.at[:, cols[k]], stin.at[:, cols[k]], xs.at[k], xr.at[k], sec, mem).wait_recv()

    states = stin[...]
    normed = rms_scale(states, gain[...]).astype(BF16)

    table_b = table.astype(BF16)
    for k in range(K):
        packed = lax.dot_general(
            table_b, normed[:, k * Dc : (k + 1) * Dc], (((0,), (0,)), ((), ())),
            preferred_element_type=F32,
        ).reshape(E, R, Dc)
        pack[:, :, cols[k]] = packed.astype(BF16)
        for d in range(1, E):
            pe = (e + d) % E
            copy = remote(
                pack.at[pe, :, cols[k]], xbuf.at[c, j, e, :, cols[k]],
                dz.at[0, k, d], dz.at[1, k, d], sec, member(pe, j, c),
            )
            copy.start()
            sends.append(copy)
        xbuf[c, j, e, :, cols[k]] = pack[e, :, cols[k]]

    logits = lax.dot_general(
        normed, router[...], (((1,), (1,)), ((), ())), preferred_element_type=F32
    )
    spread = jnp.zeros((MT, E * R), F32)
    for i in range(E):
        spread = jnp.where(lanes // R == i, logits[:, i : i + 1], spread)
    weight = jax.nn.sigmoid(spread) * table
    weight = weight / jnp.sum(weight, -1, keepdims=True)
    weight_hi = weight.astype(BF16)
    weight_lo = (weight - weight_hi.astype(F32)).astype(BF16)

    for k in range(K):
        for d in range(1, E):
            se = (e + E - d) % E
            remote(
                pack.at[se, :, cols[k]], xbuf.at[c, j, se, :, cols[k]],
                dz.at[0, k, d], dz.at[1, k, d], sec, member(se, j, c),
            ).wait_recv()
        for d in range(1, J):
            copy = remote(
                xbuf.at[c, j, :, :, cols[k]], xbuf.at[c, j, :, :, cols[k]],
                dy.at[0, k, d], dy.at[1, k, d], sec, member(e, (j + d) % J, c),
            )
            copy.start()
            sends.append(copy)
    for k in range(K):
        for d in range(1, J):
            sj = (j + J - d) % J
            remote(
                xbuf.at[c, sj, :, :, cols[k]], xbuf.at[c, sj, :, :, cols[k]],
                dy.at[0, k, d], dy.at[1, k, d], sec, member(e, sj, c),
            ).wait_recv()
        for d in range(1, C):
            copy = remote(
                xbuf.at[c, :, :, :, cols[k]], xbuf.at[c, :, :, :, cols[k]],
                dc.at[0, k, d], dc.at[1, k, d], sec, member(e, j, (c + d) % C),
            )
            copy.start()
            sends.append(copy)

    locals_[0].wait()
    locals_[1].wait()
    gate_val = up_val = None
    for k in range(K):
        for d in range(1, C):
            sc = (c + C - d) % C
            remote(
                xbuf.at[sc, :, :, :, cols[k]], xbuf.at[sc, :, :, :, cols[k]],
                dc.at[0, k, d], dc.at[1, k, d], sec, member(e, j, sc),
            ).wait_recv()
        flat = xbuf[:, :, :, :, cols[k]].astype(F32).reshape(C * J * E * R, Dc).astype(BF16)
        g = jnp.dot(flat, wg[cols[k], :], preferred_element_type=F32)
        u = jnp.dot(flat, wu[cols[k], :], preferred_element_type=F32)
        gate_val = g if gate_val is None else gate_val + g
        up_val = u if up_val is None else up_val + u
    inner = (jax.nn.silu(gate_val) * up_val).astype(BF16)

    locals_[2].wait()
    for k in range(K):
        part = jnp.dot(inner, wd[:, cols[k]], preferred_element_type=F32)
        pf[:, :, :, :, cols[k]] = part.reshape(C, J, E, R, Dc)
        for d in range(1, C):
            pc = (c + d) % C
            pb[d, :, :, :, cols[k]] = pf[pc, :, :, :, cols[k]].astype(BF16)
            copy = remote(
                pb.at[d, :, :, :, cols[k]], cr.at[d, :, :, :, cols[k]],
                rc.at[0, k, d], rc.at[1, k, d], sec, member(e, j, pc),
            )
            copy.start()
            sends.append(copy)
    for k in range(K):
        total = pf[c, :, :, :, cols[k]]
        for d in range(1, C):
            remote(
                pb.at[d, :, :, :, cols[k]], cr.at[d, :, :, :, cols[k]],
                rc.at[0, k, d], rc.at[1, k, d], sec, member(e, j, (c + C - d) % C),
            ).wait_recv()
            total = total + cr[d, :, :, :, cols[k]].astype(F32)
        qf[:, :, :, cols[k]] = total
        for d in range(1, J):
            pj = (j + d) % J
            qb[d, :, :, cols[k]] = qf[pj, :, :, cols[k]].astype(BF16)
            copy = remote(
                qb.at[d, :, :, cols[k]], yr.at[d, :, :, cols[k]],
                ry.at[0, k, d], ry.at[1, k, d], sec, member(e, pj, c),
            )
            copy.start()
            sends.append(copy)
    for k in range(K):
        total = qf[j, :, :, cols[k]]
        for d in range(1, J):
            remote(
                qb.at[d, :, :, cols[k]], yr.at[d, :, :, cols[k]],
                ry.at[0, k, d], ry.at[1, k, d], sec, member(e, (j + J - d) % J, c),
            ).wait_recv()
            total = total + yr[d, :, :, cols[k]].astype(F32)
        sb[:, :, cols[k]] = total.astype(BF16)
        for d in range(1, E):
            pe = (e + d) % E
            copy = remote(
                sb.at[pe, :, cols[k]], ret.at[e, :, cols[k]],
                rz.at[0, k, d], rz.at[1, k, d], sec, member(pe, j, c),
            )
            copy.start()
            sends.append(copy)
        ret[e, :, cols[k]] = sb[e, :, cols[k]]

    def hand_on(k):
        return remote(stout.at[:, cols[k]], stin.at[:, cols[k]], xs.at[k], xr.at[k], sec + 1, mem)

    def spread_out(k, d):
        return remote(
            fin.at[c, j, e, :, cols[k]], fin.at[c, j, e, :, cols[k]],
            fs.at[k, d], fr.at[k], sec - d, mem,
        )

    for k in range(K):
        for d in range(1, E):
            se = (e + E - d) % E
            remote(
                sb.at[se, :, cols[k]], ret.at[se, :, cols[k]],
                rz.at[0, k, d], rz.at[1, k, d], sec, member(se, j, c),
            ).wait_recv()
        back = ret[:, :, cols[k]].astype(F32).reshape(E * R, Dc).astype(BF16)
        mixed = jnp.dot(weight_hi, back, preferred_element_type=F32) + jnp.dot(
            weight_lo, back, preferred_element_type=F32
        )
        result = (states[:, k * Dc : (k + 1) * Dc].astype(F32) + 2.5 * mixed).astype(BF16)

        @pl.when(sec < S - 1)
        def _():
            stout[:, cols[k]] = result
            hand_on(k).start()

        @pl.when(sec == S - 1)
        def _():
            fin[c, j, e, :, cols[k]] = result
            for d in range(1, S):
                spread_out(k, d).start()

    for k in range(K):
        @pl.when(sec < S - 1)
        def _():
            spread_out(k, 0).wait_recv()

        for d in range(1, E):
            copy = remote(
                fin.at[c, j, e, :, cols[k]], fin.at[c, j, e, :, cols[k]],
                az.at[0, k, d], az.at[1, k, d], sec, member((e + d) % E, j, c),
            )
            copy.start()
            sends.append(copy)
    for k in range(K):
        for d in range(1, E):
            se = (e + E - d) % E
            remote(
                fin.at[c, j, se, :, cols[k]], fin.at[c, j, se, :, cols[k]],
                az.at[0, k, d], az.at[1, k, d], sec, member(se, j, c),
            ).wait_recv()
        for d in range(1, J):
            copy = remote(
                fin.at[c, j, :, :, cols[k]], fin.at[c, j, :, :, cols[k]],
                ay.at[0, k, d], ay.at[1, k, d], sec, member(e, (j + d) % J, c),
            )
            copy.start()
            sends.append(copy)
    for k in range(K):
        for d in range(1, J):
            sj = (j + J - d) % J
            remote(
                fin.at[c, sj, :, :, cols[k]], fin.at[c, sj, :, :, cols[k]],
                ay.at[0, k, d], ay.at[1, k, d], sec, member(e, sj, c),
            ).wait_recv()
        for d in range(1, C):
            copy = remote(
                fin.at[c, :, :, :, cols[k]], fin.at[c, :, :, :, cols[k]],
                ac.at[0, k, d], ac.at[1, k, d], sec, member(e, j, (c + d) % C),
            )
            copy.start()
            sends.append(copy)
    for k in range(K):
        for d in range(1, C):
            sc = (c + C - d) % C
            remote(
                fin.at[sc, :, :, :, cols[k]], fin.at[sc, :, :, :, cols[k]],
                ac.at[0, k, d], ac.at[1, k, d], sec, member(e, j, sc),
            ).wait_recv()

    for pc in range(C):
        for pj in range(J):
            block = fin[pc, pj].reshape(E * MT, D)
            base = (pc * J + pj) * E * MT
            nb[base : base + E * MT, :] = rms_scale(block, fgain[...]).astype(BF16)
    locals_[3].wait()
    scores = lax.dot_general(
        head[...], nb[...], (((1,), (1,)), ((), ())), preferred_element_type=F32
    )
    vocab = me * voc + lax.broadcasted_iota(jnp.int32, (voc, NT), 0)
    own_target = jnp.sum(jnp.where(vocab == tgt[...], scores, 0.0), 0, keepdims=True)
    own_max = jnp.max(scores, 0, keepdims=True)
    own_sum = jnp.sum(jnp.exp(scores - own_max), 0, keepdims=True)
    stats[me, :, 0:NT] = own_max
    stats[me, :, NT : 2 * NT] = own_sum
    stats[me, :, 2 * NT : 3 * NT] = own_target

    def tell(d):
        peer = (me + d) % N
        return remote(
            stats.at[me], stats.at[me], ss.at[d], sr.at[d], peer // members, peer % members
        )

    def hear(d):
        peer = (me + N - d) % N
        return remote(
            stats.at[peer], stats.at[peer], ss.at[d], sr.at[d], peer // members, peer % members
        )

    def tell_all(d, carry):
        tell(d).start()
        return carry

    def hear_all(d, carry):
        hear(d).wait_recv()
        return carry

    lax.fori_loop(1, N, tell_all, 0)
    lax.fori_loop(1, N, hear_all, 0)
    maxes = stats[:, :, 0:NT]
    peak = jnp.max(maxes, 0)
    total = jnp.sum(jnp.exp(maxes - peak[None]) * stats[:, :, NT : 2 * NT], 0)
    target_logit = jnp.sum(stats[:, :, 2 * NT : 3 * NT], 0)
    logprob = target_logit - (peak + jnp.log(total))

    own = ((c * J + j) * E + e) * MT
    lane = lax.broadcasted_iota(jnp.int32, (MT, NT), 1)
    row = lax.broadcasted_iota(jnp.int32, (MT, NT), 0)
    tok_out[...] = jnp.sum(jnp.where(lane == own + row, logprob, 0.0), -1, keepdims=True)
    lane = lax.broadcasted_iota(jnp.int32, (M * SEQS, NT), 1)
    row = lax.broadcasted_iota(jnp.int32, (M * SEQS, NT), 0)
    inside = ((lane % MT) // T == row // SEQS) & (seq[...] == row % SEQS)
    sums = jnp.sum(jnp.where(inside, logprob, 0.0), -1, keepdims=True)
    counts = jnp.sum(jnp.where(inside, 1.0, 0.0), -1, keepdims=True)
    seq_out[...] = sums / counts

    for copy in sends:
        copy.wait_send()

    @pl.when(sec < S - 1)
    def _():
        for k in range(K):
            hand_on(k).wait_send()

    @pl.when(sec == S - 1)
    def _():
        for k in range(K):
            for d in range(1, S):
                spread_out(k, d).wait_send()

    def told_all(d, carry):
        tell(d).wait_send()
        return carry

    lax.fori_loop(1, N, told_all, 0)


def body(
    hidden_in, layer_gain, router, w_gate, w_up, w_down, final_gain, head, routing, targets, seq_ids
):
    M, T, D = hidden_in.shape
    E = router.shape[2]
    top = routing.shape[3]
    S = lax.axis_size("section")
    members = lax.axis_size("expert")
    F = members // E
    C = 2 if F % 2 == 0 else 1
    J = F // C
    cap = min(T, 9 * T * top // (8 * E))
    R = -(-M * cap // 8) * 8
    K = CHUNKS
    MT = M * T
    NT = members * MT
    ff = w_gate.shape[2]
    voc = head.shape[0]
    N = S * members
    dims = (S, E, J, C, R, M, T, cap, K)

    both = jnp.stack([targets, seq_ids]).reshape(2, M, E, J, C, T)
    both = both.transpose(0, 4, 3, 2, 1, 5).reshape(2, NT)

    vmem = pl.BlockSpec(memory_space=pltpu.VMEM)
    hbm = pl.BlockSpec(memory_space=pl.ANY)
    dma = pltpu.SemaphoreType.DMA
    tok, seq = pl.pallas_call(
        functools.partial(kernel, dims),
        out_shape=(
            jax.ShapeDtypeStruct((MT, 1), F32),
            jax.ShapeDtypeStruct((M * SEQS, 1), F32),
        ),
        in_specs=[hbm, vmem, vmem, hbm, hbm, hbm, vmem, hbm, vmem, vmem, vmem],
        out_specs=(vmem, vmem),
        scratch_shapes=[
            pltpu.VMEM((D, ff), BF16),
            pltpu.VMEM((D, ff), BF16),
            pltpu.VMEM((ff, D), BF16),
            pltpu.VMEM((voc, D), BF16),
            pltpu.VMEM((MT, D), BF16),
            pltpu.VMEM((MT, D), BF16),
            pltpu.VMEM((E, R, D), BF16),
            pltpu.VMEM((C, J, E, R, D), BF16),
            pltpu.VMEM((C, J, E, R, D), F32),
            pltpu.VMEM((C, J, E, R, D), BF16),
            pltpu.VMEM((C, J, E, R, D), BF16),
            pltpu.VMEM((J, E, R, D), F32),
            pltpu.VMEM((J, E, R, D), BF16),
            pltpu.VMEM((J, E, R, D), BF16),
            pltpu.VMEM((E, R, D), BF16),
            pltpu.VMEM((E, R, D), BF16),
            pltpu.VMEM((C, J, E, MT, D), BF16),
            pltpu.VMEM((NT, D), BF16),
            pltpu.VMEM((N, 1, 3 * NT), F32),
            dma((5,)),
            dma((2, K, E)),
            dma((2, K, J)),
            dma((2, K, C)),
            dma((2, K, C)),
            dma((2, K, J)),
            dma((2, K, E)),
            dma((K,)),
            dma((K,)),
            dma((K, S)),
            dma((K,)),
            dma((2, K, E)),
            dma((2, K, J)),
            dma((2, K, C)),
            dma((N,)),
            dma((N,)),
        ],
        compiler_params=pltpu.CompilerParams(
            collective_id=0, has_side_effects=True, vmem_limit_bytes=60 * 1024 * 1024
        ),
        name="relay_experts",
    )(
        hidden_in.reshape(MT, D),
        layer_gain,
        router[0].T,
        w_gate[0],
        w_up[0],
        w_down[0],
        final_gain.reshape(1, D),
        head,
        routing[0].reshape(MT, top),
        both[0:1],
        both[1:2],
    )
    return tok.reshape(M, T), seq.reshape(M, SEQS)


def solution(mesh):
    return jax.shard_map(
        body,
        mesh=mesh,
        in_specs=(
            P(None, "expert", None),
            P("section", None),
            P("section", None, None),
            P("section", None, "expert"),
            P("section", None, "expert"),
            P("section", "expert", None),
            P(),
            P(("section", "expert"), None),
            P("section", None, "expert", None),
            P(),
            P(),
        ),
        out_specs=(P(None, "expert"), P()),
        check_vma=False,
    )
```

```python
import functools

import jax
import jax.numpy as jnp
from jax import lax
from jax.experimental import pallas as pl
from jax.experimental.pallas import tpu as pltpu
from jax.sharding import PartitionSpec as P

SEQS = 4
CHUNKS = 4
PAIR_FIRST = 1
F32 = jnp.float32
BF16 = jnp.bfloat16


def rms_scale(states, gain):
    values = states.astype(F32)
    factor = lax.rsqrt(jnp.mean(values * values, -1, keepdims=True) + 1e-06)
    return values * factor * gain


def kernel(
    dims,
    hid, gain, router, wg_hbm, wu_hbm, wd_hbm, fgain, head_hbm, route, tgt, seq,
    tok_out, seq_out,
    wg, wu, wd, head, stin, stout, pack, xbuf, pf, pb, cr, qf, qb, yr, sb, ret, fin, nb, stats, merged,
    loc, dz, dy, dc, rc, ry, rz, xs, xr, fs, fr, az, ay, ac, ss, sr, ms, mr,
):
    S, E, J, C, R, M, T, cap, K = dims
    F = J * C
    members = E * F
    MT = M * T
    D = stin.shape[1]
    Dc = D // K
    NT = members * MT
    sec = lax.axis_index("section")
    mem = lax.axis_index("expert")
    e = mem // F
    j = (mem % F) // C
    c = mem % C
    me = sec * members + mem
    voc = head.shape[0]
    cols = [pl.ds(k * Dc, Dc) for k in range(K)]

    def member(pe, pj, pc):
        return pe * F + pj * C + pc

    def remote(src, dst, send, recv, section, target):
        return pltpu.make_async_remote_copy(
            src_ref=src, dst_ref=dst, send_sem=send, recv_sem=recv,
            device_id=(section, target), device_id_type=pl.DeviceIdType.MESH,
        )

    locals_ = [
        pltpu.make_async_copy(wg_hbm, wg, loc.at[0]),
        pltpu.make_async_copy(wu_hbm, wu, loc.at[1]),
        pltpu.make_async_copy(wd_hbm, wd, loc.at[2]),
        pltpu.make_async_copy(head_hbm, head, loc.at[3]),
    ]
    load_hid = pltpu.make_async_copy(hid, stin, loc.at[4])

    @pl.when(sec == 0)
    def _():
        load_hid.start()

    for copy in locals_:
        copy.start()

    barrier = pltpu.get_barrier_semaphore()

    group = S * F
    place_in = sec * F + mem % F

    def group_peer(d):
        other = (place_in + d) % group
        return other, other // F, e * F + other % F

    def greet(d, carry):
        other, other_sec, other_mem = group_peer(d)
        pl.semaphore_signal(
            barrier, inc=1, device_id=(other_sec, other_mem),
            device_id_type=pl.DeviceIdType.MESH,
        )
        return carry

    lax.fori_loop(1, group, greet, 0)
    for d in range(1, E):
        pl.semaphore_signal(
            barrier, inc=1, device_id=(sec, member((e + d) % E, j, c)),
            device_id_type=pl.DeviceIdType.MESH,
        )

    rows = lax.broadcasted_iota(jnp.int32, (E * R, MT), 0)
    lanes = lax.broadcasted_iota(jnp.int32, (E * R, MT), 1)
    from_row = lax.broadcasted_iota(jnp.int32, (T, MT), 0)
    to_lane = lax.broadcasted_iota(jnp.int32, (T, MT), 1)
    chosen = None
    for m in range(M):
        lift = (to_lane == from_row + m * T).astype(BF16)
        ids = jnp.dot(route[m].astype(F32).astype(BF16), lift, preferred_element_type=F32)
        chosen = ids if chosen is None else chosen + ids
    row_expert = (rows // R).astype(F32)
    hit = chosen[0:1, :] == row_expert
    for k in range(1, chosen.shape[0]):
        hit = hit | (chosen[k : k + 1, :] == row_expert)
    row_a = lax.broadcasted_iota(jnp.int32, (MT, MT), 0)
    row_b = lax.broadcasted_iota(jnp.int32, (MT, MT), 1)
    earlier = ((row_a < row_b) & (row_a // T == row_b // T)).astype(BF16)
    rank = jnp.dot(hit.astype(BF16), earlier, preferred_element_type=F32)
    place = rank + ((lanes // T) * cap).astype(F32)
    table = jnp.where(hit & (place == (rows % R).astype(F32)), 1.0, 0.0).astype(F32)

    pl.semaphore_wait(barrier, group - 1 + E - 1)

    sends = []

    @pl.when(sec == 0)
    def _():
        load_hid.wait()

    @pl.when(sec > 0)
    def _():
        for k in range(K):
            remote(stout.at[:, cols[k]], stin.at[:, cols[k]], xs.at[k], xr.at[k], sec, mem).wait_recv()

    states = stin[...]
    normed = rms_scale(states, gain[...]).astype(BF16)

    table_b = table.astype(BF16)
    for k in range(K):
        packed = jnp.dot(
            table_b, normed[:, k * Dc : (k + 1) * Dc], preferred_element_type=F32
        ).reshape(E, R, Dc)
        pack[:, :, cols[k]] = packed.astype(BF16)
        for d in range(1, E):
            pe = (e + d) % E
            copy = remote(
                pack.at[pe, :, cols[k]], xbuf.at[c, j, e, :, cols[k]],
                dz.at[0, k, d], dz.at[1, k, d], sec, member(pe, j, c),
            )
            copy.start()
            sends.append(copy)
        xbuf[c, j, e, :, cols[k]] = pack[e, :, cols[k]]

    logits = lax.dot_general(
        router[...], normed, (((1,), (1,)), ((), ())), preferred_element_type=F32
    )
    spread = jnp.zeros((E * R, MT), F32)
    for i in range(E):
        spread = jnp.where(rows // R == i, logits[i : i + 1, :], spread)
    weight = jax.nn.sigmoid(spread) * table
    weight = weight / jnp.sum(weight, 0, keepdims=True)
    weight = weight.T
    weight_hi = weight.astype(BF16)
    weight_lo = (weight - weight_hi.astype(F32)).astype(BF16)

    for k in range(K):
        for d in range(1, E):
            se = (e + E - d) % E
            remote(
                pack.at[se, :, cols[k]], xbuf.at[c, j, se, :, cols[k]],
                dz.at[0, k, d], dz.at[1, k, d], sec, member(se, j, c),
            ).wait_recv()
        for d in range(1, J):
            copy = remote(
                xbuf.at[c, j, :, :, cols[k]], xbuf.at[c, j, :, :, cols[k]],
                dy.at[0, k, d], dy.at[1, k, d], sec, member(e, (j + d) % J, c),
            )
            copy.start()
            sends.append(copy)
    for k in range(K):
        for d in range(1, J):
            sj = (j + J - d) % J
            remote(
                xbuf.at[c, sj, :, :, cols[k]], xbuf.at[c, sj, :, :, cols[k]],
                dy.at[0, k, d], dy.at[1, k, d], sec, member(e, sj, c),
            ).wait_recv()
        for d in range(1, C):
            copy = remote(
                xbuf.at[c, :, :, :, cols[k]], xbuf.at[c, :, :, :, cols[k]],
                dc.at[0, k, d], dc.at[1, k, d], sec, member(e, j, (c + d) % C),
            )
            copy.start()
            sends.append(copy)

    locals_[0].wait()
    locals_[1].wait()
    gate_val = up_val = None
    for k in range(K):
        for d in range(1, C):
            sc = (c + C - d) % C
            remote(
                xbuf.at[sc, :, :, :, cols[k]], xbuf.at[sc, :, :, :, cols[k]],
                dc.at[0, k, d], dc.at[1, k, d], sec, member(e, j, sc),
            ).wait_recv()
        flat = xbuf[:, :, :, :, cols[k]].astype(F32).reshape(C * J * E * R, Dc).astype(BF16)
        g = jnp.dot(flat, wg[cols[k], :], preferred_element_type=F32)
        u = jnp.dot(flat, wu[cols[k], :], preferred_element_type=F32)
        gate_val = g if gate_val is None else gate_val + g
        up_val = u if up_val is None else up_val + u
    inner = (jax.nn.silu(gate_val) * up_val).astype(BF16)

    locals_[2].wait()
    for k in range(K):
        part = jnp.dot(inner, wd[:, cols[k]], preferred_element_type=F32)
        pf[:, :, :, :, cols[k]] = part.reshape(C, J, E, R, Dc)
        for d in range(1, C):
            pc = (c + d) % C
            pb[d, :, :, :, cols[k]] = pf[pc, :, :, :, cols[k]].astype(BF16)
            copy = remote(
                pb.at[d, :, :, :, cols[k]], cr.at[d, :, :, :, cols[k]],
                rc.at[0, k, d], rc.at[1, k, d], sec, member(e, j, pc),
            )
            copy.start()
            sends.append(copy)
    for k in range(K):
        total = pf[c, :, :, :, cols[k]]
        for d in range(1, C):
            remote(
                pb.at[d, :, :, :, cols[k]], cr.at[d, :, :, :, cols[k]],
                rc.at[0, k, d], rc.at[1, k, d], sec, member(e, j, (c + C - d) % C),
            ).wait_recv()
            total = total + cr[d, :, :, :, cols[k]].astype(F32)
        qf[:, :, :, cols[k]] = total
        for d in range(1, J):
            pj = (j + d) % J
            qb[d, :, :, cols[k]] = qf[pj, :, :, cols[k]].astype(BF16)
            copy = remote(
                qb.at[d, :, :, cols[k]], yr.at[d, :, :, cols[k]],
                ry.at[0, k, d], ry.at[1, k, d], sec, member(e, pj, c),
            )
            copy.start()
            sends.append(copy)
    for k in range(K):
        total = qf[j, :, :, cols[k]]
        for d in range(1, J):
            remote(
                qb.at[d, :, :, cols[k]], yr.at[d, :, :, cols[k]],
                ry.at[0, k, d], ry.at[1, k, d], sec, member(e, (j + J - d) % J, c),
            ).wait_recv()
            total = total + yr[d, :, :, cols[k]].astype(F32)
        sb[:, :, cols[k]] = total.astype(BF16)
        for d in range(1, E):
            pe = (e + d) % E
            copy = remote(
                sb.at[pe, :, cols[k]], ret.at[e, :, cols[k]],
                rz.at[0, k, d], rz.at[1, k, d], sec, member(pe, j, c),
            )
            copy.start()
            sends.append(copy)
        ret[e, :, cols[k]] = sb[e, :, cols[k]]

    def hand_on(k):
        return remote(stout.at[:, cols[k]], stin.at[:, cols[k]], xs.at[k], xr.at[k], sec + 1, mem)

    def spread_out(k, d):
        return remote(
            fin.at[c, j, e, :, cols[k]], fin.at[c, j, e, :, cols[k]],
            fs.at[k, d], fr.at[k], sec - d, mem,
        )

    def column(k, b):
        if k < PAIR_FIRST:
            return fin.at[c, :, b, :, cols[k]]
        return fin.at[c, j, b, :, cols[k]]

    def to_experts(k, d):
        return remote(
            column(k, e), column(k, e), az.at[0, k, d], az.at[1, k, d],
            sec, member((e + d) % E, j, c),
        )

    def from_experts(k, d):
        se = (e + E - d) % E
        return remote(
            column(k, se), column(k, se), az.at[0, k, d], az.at[1, k, d], sec, member(se, j, c)
        )

    def pair_ref(k, pj):
        if k < PAIR_FIRST:
            return fin.at[c, pj, e, :, cols[k]]
        return fin.at[c, pj, :, :, cols[k]]

    def to_pair(k, d):
        return remote(
            pair_ref(k, j), pair_ref(k, j), ay.at[0, k, d], ay.at[1, k, d],
            sec, member(e, (j + d) % J, c),
        )

    def from_pair(k, d):
        sj = (j + J - d) % J
        return remote(
            pair_ref(k, sj), pair_ref(k, sj), ay.at[0, k, d], ay.at[1, k, d],
            sec, member(e, sj, c),
        )

    def launch(k):
        if k < PAIR_FIRST:
            for d in range(1, J):
                to_pair(k, d).start()
        else:
            for d in range(1, E):
                to_experts(k, d).start()

    for k in range(K):
        for d in range(1, E):
            se = (e + E - d) % E
            remote(
                sb.at[se, :, cols[k]], ret.at[se, :, cols[k]],
                rz.at[0, k, d], rz.at[1, k, d], sec, member(se, j, c),
            ).wait_recv()
        back = ret[:, :, cols[k]].astype(F32).reshape(E * R, Dc).astype(BF16)
        mixed = jnp.dot(weight_hi, back, preferred_element_type=F32) + jnp.dot(
            weight_lo, back, preferred_element_type=F32
        )
        result = (states[:, k * Dc : (k + 1) * Dc].astype(F32) + 2.5 * mixed).astype(BF16)

        @pl.when(sec < S - 1)
        def _():
            stout[:, cols[k]] = result
            hand_on(k).start()

        @pl.when(sec == S - 1)
        def _():
            fin[c, j, e, :, cols[k]] = result
            for d in range(1, S):
                spread_out(k, d).start()
            launch(k)

    @pl.when(sec < S - 1)
    def _():
        for k in range(K):
            spread_out(k, 0).wait_recv()
            launch(k)

    for k in range(PAIR_FIRST):
        for d in range(1, J):
            from_pair(k, d).wait_recv()
        for d in range(1, E):
            to_experts(k, d).start()
    late = list(range(PAIR_FIRST, K)) + list(range(PAIR_FIRST))
    for k in late:
        for d in range(1, E):
            from_experts(k, d).wait_recv()
        if k >= PAIR_FIRST:
            for d in range(1, J):
                to_pair(k, d).start()
    for k in late[::-1]:
        if k >= PAIR_FIRST:
            for d in range(1, J):
                from_pair(k, d).wait_recv()
        for d in range(1, C):
            copy = remote(
                fin.at[c, :, :, :, cols[k]], fin.at[c, :, :, :, cols[k]],
                ac.at[0, k, d], ac.at[1, k, d], sec, member(e, j, (c + d) % C),
            )
            copy.start()
            sends.append(copy)
    for k in range(K):
        for d in range(1, C):
            sc = (c + C - d) % C
            remote(
                fin.at[sc, :, :, :, cols[k]], fin.at[sc, :, :, :, cols[k]],
                ac.at[0, k, d], ac.at[1, k, d], sec, member(e, j, sc),
            ).wait_recv()

    for pj in range(J):
        for pe in range(E):
            blocks = [
                rms_scale(fin[pc, pj, pe], fgain[...].reshape(1, D)) for pc in range(C)
            ]
            for m in range(M):
                base = m * members * T + member(pe, pj, 0) * T
                piece = jnp.concatenate([b[m * T : (m + 1) * T, :] for b in blocks], 0)
                nb[base : base + C * T, :] = piece.astype(BF16)
    locals_[3].wait()
    scores = lax.dot_general(
        head[...], nb[...], (((1,), (1,)), ((), ())), preferred_element_type=F32
    )
    vocab = me * voc + lax.broadcasted_iota(jnp.int32, (voc, NT), 0)
    aims = jnp.concatenate([tgt[m : m + 1, :] for m in range(M)], 1)
    own_target = jnp.sum(jnp.where(vocab == aims, scores, 0.0), 0, keepdims=True)
    own_max = jnp.max(scores, 0, keepdims=True)
    own_sum = jnp.sum(jnp.exp(scores - own_max), 0, keepdims=True)
    def put(ref, at, values):
        for i, value in enumerate(values):
            ref[at, :, i * NT : (i + 1) * NT] = value

    def merge(ref):
        maxes = ref[:, :, 0:NT]
        top = jnp.max(maxes, 0)
        total = jnp.sum(jnp.exp(maxes - top[None]) * ref[:, :, NT : 2 * NT], 0)
        return top, total, jnp.sum(ref[:, :, 2 * NT : 3 * NT], 0)

    put(stats, place_in, (own_max, own_sum, own_target))

    def tell(d):
        other, other_sec, other_mem = group_peer(d)
        return remote(
            stats.at[place_in], stats.at[place_in], ss.at[d], sr.at[d], other_sec, other_mem
        )

    def hear(d):
        other, other_sec, other_mem = group_peer(group - d)
        return remote(stats.at[other], stats.at[other], ss.at[d], sr.at[d], other_sec, other_mem)

    def tell_all(d, carry):
        tell(d).start()
        return carry

    def hear_all(d, carry):
        hear(d).wait_recv()
        return carry

    lax.fori_loop(1, group, tell_all, 0)
    lax.fori_loop(1, group, hear_all, 0)
    put(merged, e, merge(stats))
    for d in range(1, E):
        copy = remote(
            merged.at[e], merged.at[e], ms.at[d], mr.at[d], sec, member((e + d) % E, j, c)
        )
        copy.start()
        sends.append(copy)
    for d in range(1, E):
        se = (e + E - d) % E
        remote(
            merged.at[se], merged.at[se], ms.at[d], mr.at[d], sec, member(se, j, c)
        ).wait_recv()
    peak, total, target_logit = merge(merged)
    logprob = target_logit - (peak + jnp.log(total))

    def across(column, count):
        a = lax.broadcasted_iota(jnp.int32, (count, count), 0)
        b = lax.broadcasted_iota(jnp.int32, (count, count), 1)
        return jnp.sum(jnp.where(a == b, column, 0.0), 0, keepdims=True)

    tokens = members * T
    lane = lax.broadcasted_iota(jnp.int32, (T, tokens), 1)
    row = lax.broadcasted_iota(jnp.int32, (T, tokens), 0)
    row_s = lax.broadcasted_iota(jnp.int32, (SEQS, tokens), 0)
    for m in range(M):
        line = logprob[:, m * tokens : (m + 1) * tokens]
        own = jnp.sum(jnp.where(lane == mem * T + row, line, 0.0), -1, keepdims=True)
        tok_out[m : m + 1, :] = across(own, T)
        inside = seq[m : m + 1, :] == row_s
        sums = jnp.sum(jnp.where(inside, line, 0.0), -1, keepdims=True)
        counts = jnp.sum(jnp.where(inside, 1.0, 0.0), -1, keepdims=True)
        seq_out[m : m + 1, :] = across(sums / counts, SEQS)

    for copy in sends:
        copy.wait_send()

    @pl.when(sec < S - 1)
    def _():
        for k in range(K):
            hand_on(k).wait_send()

    @pl.when(sec == S - 1)
    def _():
        for k in range(K):
            for d in range(1, S):
                spread_out(k, d).wait_send()

    def told_all(d, carry):
        tell(d).wait_send()
        return carry

    lax.fori_loop(1, group, told_all, 0)
    for k in range(K):
        for d in range(1, E):
            to_experts(k, d).wait_send()
        for d in range(1, J):
            to_pair(k, d).wait_send()


def body(
    hidden_in, layer_gain, router, w_gate, w_up, w_down, final_gain, head, routing, targets, seq_ids
):
    M, T, D = hidden_in.shape
    E = router.shape[2]
    top = routing.shape[3]
    S = lax.axis_size("section")
    members = lax.axis_size("expert")
    F = members // E
    C = 2 if F % 2 == 0 else 1
    J = F // C
    cap = min(T, 9 * T * top // (8 * E))
    R = -(-M * cap // 8) * 8
    K = CHUNKS
    MT = M * T
    NT = members * MT
    ff = w_gate.shape[2]
    voc = head.shape[0]
    dims = (S, E, J, C, R, M, T, cap, K)

    vmem = pl.BlockSpec(memory_space=pltpu.VMEM)
    hbm = pl.BlockSpec(memory_space=pl.ANY)
    dma = pltpu.SemaphoreType.DMA
    tok, seq = pl.pallas_call(
        functools.partial(kernel, dims),
        out_shape=(
            jax.ShapeDtypeStruct((M, T), F32),
            jax.ShapeDtypeStruct((M, SEQS), F32),
        ),
        in_specs=[hbm, vmem, vmem, hbm, hbm, hbm, vmem, hbm, vmem, vmem, vmem],
        out_specs=(vmem, vmem),
        scratch_shapes=[
            pltpu.VMEM((D, ff), BF16),
            pltpu.VMEM((D, ff), BF16),
            pltpu.VMEM((ff, D), BF16),
            pltpu.VMEM((voc, D), BF16),
            pltpu.VMEM((MT, D), BF16),
            pltpu.VMEM((MT, D), BF16),
            pltpu.VMEM((E, R, D), BF16),
            pltpu.VMEM((C, J, E, R, D), BF16),
            pltpu.VMEM((C, J, E, R, D), F32),
            pltpu.VMEM((C, J, E, R, D), BF16),
            pltpu.VMEM((C, J, E, R, D), BF16),
            pltpu.VMEM((J, E, R, D), F32),
            pltpu.VMEM((J, E, R, D), BF16),
            pltpu.VMEM((J, E, R, D), BF16),
            pltpu.VMEM((E, R, D), BF16),
            pltpu.VMEM((E, R, D), BF16),
            pltpu.VMEM((C, J, E, MT, D), BF16),
            pltpu.VMEM((NT, D), BF16),
            pltpu.VMEM((S * F, 1, 3 * NT), F32),
            pltpu.VMEM((E, 1, 3 * NT), F32),
            dma((5,)),
            dma((2, K, E)),
            dma((2, K, J)),
            dma((2, K, C)),
            dma((2, K, C)),
            dma((2, K, J)),
            dma((2, K, E)),
            dma((K,)),
            dma((K,)),
            dma((K, S)),
            dma((K,)),
            dma((2, K, E)),
            dma((2, K, J)),
            dma((2, K, C)),
            dma((S * F,)),
            dma((S * F,)),
            dma((E,)),
            dma((E,)),
        ],
        compiler_params=pltpu.CompilerParams(
            collective_id=0, has_side_effects=True, vmem_limit_bytes=60 * 1024 * 1024
        ),
        name="relay_experts",
    )(
        hidden_in.reshape(MT, D),
        layer_gain,
        router[0].T,
        w_gate[0],
        w_up[0],
        w_down[0],
        final_gain,
        head,
        routing[0].transpose(0, 2, 1),
        targets,
        seq_ids,
    )
    return tok, seq


def solution(mesh):
    return jax.shard_map(
        body,
        mesh=mesh,
        in_specs=(
            P(None, "expert", None),
            P("section", None),
            P("section", None, None),
            P("section", None, "expert"),
            P("section", None, "expert"),
            P("section", "expert", None),
            P(),
            P(("section", "expert"), None),
            P("section", None, "expert", None),
            P(),
            P(),
        ),
        out_specs=(P(None, "expert"), P()),
        check_vma=False,
    )
```
